32 devices in a mesh: grp: 4 (over z), dev: 8 (over y, x, core).
Axes of the slice: x: 2, y: 2, z: 4, core: 2. Of those that a mesh axis runs over, the one named last changes fastest.
Arguments:
- images: bfloat16 [1536, 1536], P(('grp', 'dev')), may hold values from -1 to 1, as said below
- texts: bfloat16 [1536, 1536], P(('grp', 'dev')), may hold values from -1 to 1, as said below
- logit_scale: float32 [1], replicated, may hold values from 20 to 60
- logit_bias: float32 [1], replicated, may hold values from -12 to -8
Outputs:
- grad_image: float32 [1536, 1536], P(('grp', 'dev'))
- grad_text: float32 [1536, 1536], P(('grp', 'dev'))
- loss: float32 [1], replicated
The draws below stay inside these ranges and needn't reach their ends.
Inputs may be any that keep to these rules, and one draw needn't show every extreme that they name: `images`: every row has length 1 up to bfloat16 rounding. `texts`: every row has length 1 up to bfloat16 rounding.
All inputs are finite; a program needn't handle non-finite values.
Results may differ from the reference program's by a relative error of at most 0.00095.
Values may be sent and summed in bfloat16 or wider, within the bound.
A program may use at most 128 MiB of HBM per device.

```python
import jax
import jax.numpy as jnp
from jax import lax

D = 1536
ROWS = 48
BATCH = 1536
N_DEV = 8


def unit_rows(values):
    return values / jnp.sqrt(jnp.sum(values * values, axis=-1, keepdims=True))


def paired_rows(key):
    spread = 0.65
    column_scale = jnp.exp(spread * jax.random.normal(jax.random.fold_in(key, 11), (D,), jnp.float32))
    image_raw = jax.random.normal(jax.random.fold_in(key, 12), (BATCH, D), jnp.float32)
    noise_raw = jax.random.normal(jax.random.fold_in(key, 13), (BATCH, D), jnp.float32)
    image_dir = unit_rows(image_raw * column_scale[None, :])
    noise_dir = unit_rows(noise_raw * column_scale[None, :])
    text_dir = unit_rows(0.8 * image_dir + 0.6 * noise_dir)
    return (image_dir, text_dir)


def draw_images(key, part):
    return paired_rows(key)[0].astype(jnp.bfloat16)


def draw_texts(key, part):
    return paired_rows(key)[1].astype(jnp.bfloat16)


def setup_inputs(seed: int = 0) -> dict:
    key_list = jax.random.split(jax.random.key(seed), 5)
    return {
        "images": draw_images(jax.random.fold_in(key_list[4], 71), 0),
        "texts": draw_texts(jax.random.fold_in(key_list[4], 71), 0),
        "logit_scale": jnp.clip(jax.random.uniform(key_list[2], (1,), jnp.float32, 20.0, 60.0), 20.0, 60.0),
        "logit_bias": jnp.clip(jax.random.uniform(key_list[3], (1,), jnp.float32, -12.0, -8.0), -12.0, -8.0),
    }


def reference(images, texts, logit_scale, logit_bias):
    logit_mult = logit_scale[0]
    logit_shift = logit_bias[0]
    pair_total = images.shape[0]
    block_rows = N_DEV * ROWS
    block_number = pair_total // block_rows
    text_ids = jnp.arange(pair_total, dtype=jnp.int32)

    def block_step(running, block_index):
        grad_texts, loss_sum = running
        first_row = (block_index * block_rows).astype(jnp.int32)
        left_rows = lax.dynamic_slice_in_dim(images, first_row, block_rows, 0)
        left_ids = first_row + jnp.arange(block_rows, dtype=jnp.int32)
        logits = jnp.dot(left_rows, texts.T, preferred_element_type=jnp.float32) * logit_mult + logit_shift
        matched = left_ids[:, None] == text_ids[None, :]
        labels = jnp.where(matched, 1.0, -1.0).astype(jnp.float32)
        loss_part = -jnp.sum(jax.nn.log_sigmoid(labels * logits))
        weights = (jax.nn.sigmoid(logits) - matched.astype(jnp.float32)).astype(jnp.bfloat16)
        grad_left = logit_mult * jnp.dot(weights, texts, preferred_element_type=jnp.float32)
        grad_texts = grad_texts + logit_mult * jnp.dot(weights.T, left_rows, preferred_element_type=jnp.float32)
        return (grad_texts, loss_sum + loss_part), grad_left

    start_state = (jnp.zeros(texts.shape, jnp.float32), jnp.zeros((), jnp.float32))
    (grad_text, loss_sum), grad_blocks = lax.scan(block_step, start_state, jnp.arange(block_number, dtype=jnp.int32))
    grad_image = grad_blocks.reshape(pair_total, images.shape[1])
    return grad_image, grad_text, (loss_sum / pair_total).reshape(1)
```

```python
import functools
import math

import jax
import jax.numpy as jnp
from jax import lax
from jax.experimental import pallas as pl
from jax.experimental.pallas import tpu as pltpu
from jax.sharding import PartitionSpec as P

MESH = pl.DeviceIdType.MESH
CORES = 2


def split_chips(members):
    chips = members // CORES
    q_size = math.isqrt(chips)
    while chips % q_size:
        q_size -= 1
    return chips // q_size, q_size


def piece_count(rows):
    for pieces in (3, 2):
        if rows % (16 * pieces) == 0:
            return pieces
    return 1


def pair_terms(logits, matched):
    small = jnp.exp(-jnp.abs(logits))
    sigmoid = jnp.where(logits >= 0, 1.0, small) / (1.0 + small)
    if matched is None:
        return sigmoid, jnp.maximum(logits, 0.0) + jnp.log1p(small)
    weights = sigmoid - matched.astype(jnp.float32)
    signed = jnp.where(matched, -logits, logits)
    return weights, jnp.maximum(signed, 0.0) + jnp.log1p(small)


def kernel(
    groups, p_size, q_size, pieces,
    img_ref, txt_ref, scale_ref, bias_ref,
    gi_ref, gt_ref, loss_ref,
    img_all, txt_all, acc_i, acc_t, part_i, part_t,
    loss_acc, loss_own, loss_dev, loss_sum, loss_grp,
    img_recv, img_z, img_plane, img_core,
    txt_recv, txt_z, txt_plane, txt_core,
    pi_send, pi_recv, pt_send, pt_recv,
    ld_send, ld_recv, lg_send, lg_recv,
):
    rows = img_ref.shape[0]
    members = p_size * q_size * CORES
    g = lax.axis_index("grp")
    d = lax.axis_index("dev")
    c = lax.rem(d, CORES)
    chip = d // CORES
    q = lax.rem(chip, q_size)
    p = chip // q_size
    step_rows = rows // pieces
    multiplier = scale_ref[0]
    offset = bias_ref[0]

    def member(pi, qi, ci):
        return (pi * q_size + qi) * CORES + ci

    barrier = pltpu.get_barrier_semaphore()
    for k in range(1, members):
        pl.semaphore_signal(barrier, inc=1, device_id={"dev": lax.rem(d + k, members)}, device_id_type=MESH)
    for k in range(1, groups):
        pl.semaphore_signal(barrier, inc=1, device_id={"grp": lax.rem(g + k, groups)}, device_id_type=MESH)
    pl.semaphore_wait(barrier, members + groups - 2)

    class Side:
        def __init__(self, own, all_ref, recv, zs, ps, cs, me, size, partner):
            self.own, self.all, self.recv = own, all_ref, recv
            self.zs, self.ps, self.cs = zs, ps, cs
            self.me, self.size, self.partner = me, size, partner

        def piece(self, gg, m, cc, h):
            return self.all.at[gg, m, cc, pl.ds(h * step_rows, step_rows)]

        def copy(self, gg, m, cc, h, send, target, own=False):
            dst = self.piece(gg, m, cc, h)
            src = self.own.at[pl.ds(h * step_rows, step_rows)] if own else dst
            return pltpu.make_async_remote_copy(
                src_ref=src, dst_ref=dst, send_sem=send, recv_sem=self.recv.at[gg, m, cc, h],
                device_id=target, device_id_type=MESH,
            )

        def arrived(self, gg, m, cc, h):
            self.copy(gg, m, cc, h, self.cs.at[0, 0, 0], {"dev": member(p, q, 1 - c)}).wait_recv()

        def along_z(self, gg, h, up, own=False):
            slot = gg if (up or not own) else groups
            return self.copy(gg, self.me, c, h, self.zs.at[slot, h], {"grp": g + 1 if up else g - 1}, own)

        def to_plane(self, gg, k, h, own=False):
            other = lax.rem(self.me + k, self.size)
            return self.copy(gg, self.me, c, h, self.ps.at[gg, k - 1, h], {"dev": self.partner(other)}, own)

        def to_core(self, gg, m, h, own=False):
            return self.copy(gg, m, c, h, self.cs.at[gg, m, h], {"dev": member(p, q, 1 - c)}, own)

    texts = Side(txt_ref, txt_all, txt_recv, txt_z, txt_plane, txt_core, q, q_size, lambda o: member(p, o, c))
    images = Side(img_ref, img_all, img_recv, img_z, img_plane, img_core, p, p_size, lambda o: member(o, q, c))
    sides = (texts, images)

    def from_side(s, down):
        return (g - s, g >= s) if not down else (g + s, g + s < groups)

    for side in sides:
        for h in range(pieces):
            @pl.when(g + 1 < groups)
            def _():
                side.along_z(g, h, True, True).start()

            @pl.when(g > 0)
            def _():
                side.along_z(g, h, False, True).start()

            for k in range(1, side.size):
                side.to_plane(g, k, h, True).start()
            side.to_core(g, side.me, h, True).start()
    txt_all[g, q, c] = txt_ref[...]
    img_all[g, p, c] = img_ref[...]

    def forward_z(s):
        for side in sides:
            for h in range(pieces):
                for down in (False, True):
                    gg, there = from_side(s, down)

                    @pl.when(there)
                    def _():
                        side.arrived(gg, side.me, c, h)

                        @pl.when((g > 0) if down else (g + 1 < groups))
                        def _():
                            side.along_z(gg, h, not down).start()

                        for k in range(1, side.size):
                            side.to_plane(gg, k, h).start()
                        side.to_core(gg, side.me, h).start()

    def each_chunk(s, act):
        if s == 0:
            act(g)
            return
        for down in (False, True):
            gg, there = from_side(s, down)

            @pl.when(there)
            def _():
                act(gg)

    def relay_plane(s):
        def act(gg):
            for side in sides:
                for h in range(pieces):
                    for k in range(1, side.size):
                        other = lax.rem(side.me + k, side.size)
                        side.arrived(gg, other, c, h)
                        side.to_core(gg, other, h).start()

        each_chunk(s, act)

    def gradient(mine, other, acc, gg, first, losses):
        width = acc.shape[2]
        left = mine.all[g, :, c].reshape(mine.size * rows, width)
        right = other.all[gg].reshape(other.size * CORES * rows, width)
        logits = lax.dot_general(left, right, (((1,), (1,)), ((), ())), preferred_element_type=jnp.float32)
        logits = logits * multiplier + offset
        matched = None
        if first:
            row = lax.broadcasted_iota(jnp.int32, logits.shape, 0) - mine.me * rows
            col = lax.broadcasted_iota(jnp.int32, logits.shape, 1) - (other.me * CORES + c) * rows
            matched = (row == col) & (row >= 0) & (row < rows)
        weights, terms = pair_terms(logits, matched)
        if losses:
            loss_acc[...] = terms if first else loss_acc[...] + terms
        product = jnp.dot(weights.astype(jnp.bfloat16), right, preferred_element_type=jnp.float32)
        product = product.reshape(mine.size, rows, width)
        acc[...] = product if first else acc[...] + product

    def compute(s):
        def act(gg):
            for side in sides:
                for m in range(side.size):
                    for h in range(pieces):
                        side.arrived(gg, m, 1 - c, h)
            gradient(images, texts, acc_i, gg, s == 0, True)
            gradient(texts, images, acc_t, gg, s == 0, False)

        each_chunk(s, act)

    for s in range(groups + 2):
        if 0 < s < groups:
            forward_z(s)
        if 0 <= s - 1 < groups:
            relay_plane(s - 1)
            compute(s - 1)

    def partial(acc, part, send, recv, side, k):
        other = lax.rem(side.me + k, side.size)
        return pltpu.make_async_remote_copy(
            src_ref=acc.at[other], dst_ref=part.at[side.me], send_sem=send.at[k - 1], recv_sem=recv.at[side.me],
            device_id={"dev": side.partner(other)}, device_id_type=MESH,
        )

    def partial_in(acc, part, send, recv, side, k):
        other = lax.rem(side.me + k, side.size)
        return pltpu.make_async_remote_copy(
            src_ref=acc.at[other], dst_ref=part.at[other], send_sem=send.at[k - 1], recv_sem=recv.at[other],
            device_id={"dev": side.partner(other)}, device_id_type=MESH,
        )

    finals = ((acc_t, part_t, pt_send, pt_recv, texts, gt_ref), (acc_i, part_i, pi_send, pi_recv, images, gi_ref))
    for acc, part, send, recv, side, _ in finals:
        for k in range(1, side.size):
            partial(acc, part, send, recv, side, k).start()

    def all_sum(value, own, gathered, send, recv, axis, me, size):
        own[...] = jnp.full(own.shape, value, jnp.float32)
        gathered[me] = own[...]

        def out(k, slot):
            return pltpu.make_async_remote_copy(
                src_ref=own, dst_ref=gathered.at[slot], send_sem=send.at[k - 1], recv_sem=recv.at[slot],
                device_id={axis: lax.rem(me + k, size)}, device_id_type=MESH,
            )

        for k in range(1, size):
            out(k, me).start()
        for k in range(1, size):
            out(k, lax.rem(me + k, size)).wait_recv()
        total = gathered[0]
        for k in range(1, size):
            total = total + gathered[k]
        for k in range(1, size):
            out(k, me).wait_send()
        return total

    total = all_sum(jnp.sum(loss_acc[...]), loss_own, loss_dev, ld_send, ld_recv, "dev", d, members)
    total = all_sum(total, loss_sum, loss_grp, lg_send, lg_recv, "grp", g, groups)
    loss_ref[...] = total * (1.0 / (rows * members * groups))

    for acc, part, send, recv, side, out_ref in finals:
        total = acc[side.me]
        for k in range(1, side.size):
            partial_in(acc, part, send, recv, side, k).wait_recv()
            total = total + part[lax.rem(side.me + k, side.size)]
        out_ref[...] = multiplier * total
        for k in range(1, side.size):
            partial(acc, part, send, recv, side, k).wait_send()

    for side in sides:
        for h in range(pieces):
            @pl.when(g + 1 < groups)
            def _():
                side.along_z(g, h, True, True).wait_send()

            @pl.when(g > 0)
            def _():
                side.along_z(g, h, False, True).wait_send()

            for s in range(groups):
                def act(gg):
                    for k in range(1, side.size):
                        side.to_plane(gg, k, h).wait_send()
                    for m in range(side.size):
                        side.to_core(gg, m, h).wait_send()

                each_chunk(s, act)
                for down in (False, True):
                    if s:
                        gg, there = from_side(s, down)

                        @pl.when(there & ((g > 0) if down else (g + 1 < groups)))
                        def _():
                            side.along_z(gg, h, not down).wait_send()


def shards(groups, members, images, texts, logit_scale, logit_bias):
    rows, width = images.shape
    p_size, q_size = split_chips(members)
    pieces = piece_count(rows)
    f32, bf16 = jnp.float32, jnp.bfloat16
    dma = pltpu.SemaphoreType.DMA

    def side_sems(size):
        return [
            dma((groups, size, CORES, pieces)),
            dma((groups + 1, pieces)),
            dma((groups, max(size - 1, 1), pieces)),
            dma((groups, size, pieces)),
        ]

    vmem, smem = pl.BlockSpec(memory_space=pltpu.VMEM), pl.BlockSpec(memory_space=pltpu.SMEM)
    grad_image, grad_text, loss = pl.pallas_call(
        functools.partial(kernel, groups, p_size, q_size, pieces),
        out_shape=(
            jax.ShapeDtypeStruct((rows, width), f32),
            jax.ShapeDtypeStruct((rows, width), f32),
            jax.ShapeDtypeStruct((8, 128), f32),
        ),
        in_specs=[vmem, vmem, smem, smem],
        out_specs=(vmem, vmem, vmem),
        scratch_shapes=[
            pltpu.VMEM((groups, p_size, CORES, rows, width), bf16),
            pltpu.VMEM((groups, q_size, CORES, rows, width), bf16),
            pltpu.VMEM((p_size, rows, width), f32),
            pltpu.VMEM((q_size, rows, width), f32),
            pltpu.VMEM((p_size, rows, width), f32),
            pltpu.VMEM((q_size, rows, width), f32),
            pltpu.VMEM((p_size * rows, q_size * CORES * rows), f32),
            pltpu.VMEM((8, 128), f32),
            pltpu.VMEM((members, 8, 128), f32),
            pltpu.VMEM((8, 128), f32),
            pltpu.VMEM((groups, 8, 128), f32),
            *side_sems(p_size),
            *side_sems(q_size),
            dma((p_size,)), dma((p_size,)), dma((q_size,)), dma((q_size,)),
            dma((members,)), dma((members,)), dma((groups,)), dma((groups,)),
        ],
        compiler_params=pltpu.CompilerParams(
            collective_id=0, has_side_effects=True, vmem_limit_bytes=60 * 1024 * 1024
        ),
    )(images, texts, logit_scale, logit_bias)
    return grad_image, grad_text, loss[0, :1]


def solution(mesh):
    in_specs = (P(("grp", "dev"), None), P(("grp", "dev"), None), P(), P())
    out_specs = (P(("grp", "dev"), None), P(("grp", "dev"), None), P())
    body = functools.partial(shards, mesh.shape["grp"], mesh.shape["dev"])
    return jax.shard_map(body, mesh=mesh, in_specs=in_specs, out_specs=out_specs, check_vma=False)
```

```python
import functools
import math

import jax
import jax.numpy as jnp
from jax import lax
from jax.experimental import pallas as pl
from jax.experimental.pallas import tpu as pltpu
from jax.sharding import PartitionSpec as P

MESH = pl.DeviceIdType.MESH
CORES = 2


def split_chips(members):
    chips = members // CORES
    q_size = math.isqrt(chips)
    while chips % q_size:
        q_size -= 1
    return chips // q_size, q_size


def piece_count(rows):
    for pieces in (3, 2):
        if rows % (16 * pieces) == 0:
            return pieces
    return 1


def pair_terms(logits, matched):
    small = jnp.exp(-jnp.abs(logits))
    sigmoid = jnp.where(logits >= 0, 1.0, small) / (1.0 + small)
    if matched is None:
        return sigmoid, jnp.maximum(logits, 0.0) + jnp.log1p(small)
    weights = sigmoid - matched.astype(jnp.float32)
    signed = jnp.where(matched, -logits, logits)
    return weights, jnp.maximum(signed, 0.0) + jnp.log1p(small)


def kernel(
    groups, p_size, q_size, pieces,
    img_hbm, txt_hbm, scale_hbm, bias_hbm,
    gi_ref, gt_ref, loss_ref,
    img_all, txt_all, acc_i, acc_t, part_i, part_t,
    loss_acc, loss_own, loss_dev, loss_sum, loss_grp,
    img_recv, img_z, img_plane, img_core,
    txt_recv, txt_z, txt_plane, txt_core,
    pi_send, pi_recv, pt_send, pt_recv,
    ld_send, ld_recv, lg_send, lg_recv,
    scale_ref, bias_ref, fetch_sem,
):
    rows = img_hbm.shape[0]
    members = p_size * q_size * CORES
    g = lax.axis_index("grp")
    d = lax.axis_index("dev")
    c = lax.rem(d, CORES)
    chip = d // CORES
    q = lax.rem(chip, q_size)
    p = chip // q_size
    step_rows = rows // pieces

    def member(pi, qi, ci):
        return (pi * q_size + qi) * CORES + ci

    fetches = [
        pltpu.make_async_copy(src, dst, fetch_sem.at[i])
        for i, (src, dst) in enumerate((
            (txt_hbm, txt_all.at[g, q, c]), (img_hbm, img_all.at[g, p, c]), (scale_hbm, scale_ref), (bias_hbm, bias_ref),
        ))
    ]
    barrier = pltpu.get_barrier_semaphore()

    def greet(axis, index):
        pl.semaphore_signal(barrier, inc=1, device_id={axis: index}, device_id_type=MESH)

    @pl.when(g + 1 < groups)
    def _():
        greet("grp", g + 1)

    @pl.when(g > 0)
    def _():
        greet("grp", g - 1)

    for k in range(1, p_size):
        greet("dev", member(lax.rem(p + k, p_size), q, c))
    for k in range(1, q_size):
        greet("dev", member(p, lax.rem(q + k, q_size), c))
    greet("dev", member(p, q, 1 - c))
    for fetch in fetches:
        fetch.start()
    edges = (g > 0).astype(jnp.int32) + (g + 1 < groups).astype(jnp.int32)
    pl.semaphore_wait(barrier, p_size + q_size - 1 + edges)

    class Side:
        def __init__(self, all_ref, recv, zs, ps, cs, me, size, partner):
            self.all, self.recv = all_ref, recv
            self.zs, self.ps, self.cs = zs, ps, cs
            self.me, self.size, self.partner = me, size, partner

        def piece(self, gg, m, cc, h):
            return self.all.at[gg, m, cc, pl.ds(h * step_rows, step_rows)]

        def copy(self, gg, m, cc, h, send, target):
            dst = self.piece(gg, m, cc, h)
            return pltpu.make_async_remote_copy(
                src_ref=dst, dst_ref=dst, send_sem=send, recv_sem=self.recv.at[gg, m, cc, h],
                device_id=target, device_id_type=MESH,
            )

        def arrived(self, gg, m, cc, h):
            self.copy(gg, m, cc, h, self.cs.at[0, 0, 0], {"dev": member(p, q, 1 - c)}).wait_recv()

        def along_z(self, gg, h, up, own=False):
            slot = gg if (up or not own) else groups
            return self.copy(gg, self.me, c, h, self.zs.at[slot, h], {"grp": g + 1 if up else g - 1})

        def to_plane(self, gg, k, h):
            other = lax.rem(self.me + k, self.size)
            return self.copy(gg, self.me, c, h, self.ps.at[gg, k - 1, h], {"dev": self.partner(other)})

        def to_core(self, gg, m, h):
            return self.copy(gg, m, c, h, self.cs.at[gg, m, h], {"dev": member(p, q, 1 - c)})

    texts = Side(txt_all, txt_recv, txt_z, txt_plane, txt_core, q, q_size, lambda o: member(p, o, c))
    images = Side(img_all, img_recv, img_z, img_plane, img_core, p, p_size, lambda o: member(o, q, c))
    sides = (texts, images)

    def from_side(s, down):
        return (g - s, g >= s) if not down else (g + s, g + s < groups)

    for side, fetch in zip(sides, fetches):
        fetch.wait()
        for h in range(pieces):
            @pl.when(g + 1 < groups)
            def _():
                side.along_z(g, h, True, True).start()

            @pl.when(g > 0)
            def _():
                side.along_z(g, h, False, True).start()

            for k in range(1, side.size):
                side.to_plane(g, k, h).start()
            side.to_core(g, side.me, h).start()
    for fetch in fetches[2:]:
        fetch.wait()
    multiplier = scale_ref[0]
    offset = bias_ref[0]

    def forward_z(s, side):
        for h in range(pieces):
            for down in (False, True):
                gg, there = from_side(s, down)

                @pl.when(there)
                def _():
                    side.arrived(gg, side.me, c, h)

                    @pl.when((g > 0) if down else (g + 1 < groups))
                    def _():
                        side.along_z(gg, h, not down).start()

                    for k in range(1, side.size):
                        side.to_plane(gg, k, h).start()
                    side.to_core(gg, side.me, h).start()

    def each_chunk(s, act):
        if s == 0:
            act(g)
            return
        for down in (False, True):
            gg, there = from_side(s, down)

            @pl.when(there)
            def _():
                act(gg)

    def relay_plane(s, side):
        def act(gg):
            for h in range(pieces):
                for k in range(1, side.size):
                    other = lax.rem(side.me + k, side.size)
                    side.arrived(gg, other, c, h)
                    side.to_core(gg, other, h).start()

        each_chunk(s, act)

    def gradient(mine, other, acc, gg, first, losses):
        width = acc.shape[2]
        left = mine.all[g, :, c].reshape(mine.size * rows, width)
        right = other.all[gg].reshape(other.size * CORES * rows, width)
        logits = lax.dot_general(left, right, (((1,), (1,)), ((), ())), preferred_element_type=jnp.float32)
        logits = logits * multiplier + offset
        matched = None
        if first:
            row = lax.broadcasted_iota(jnp.int32, logits.shape, 0) - mine.me * rows
            col = lax.broadcasted_iota(jnp.int32, logits.shape, 1) - (other.me * CORES + c) * rows
            matched = (row == col) & (row >= 0) & (row < rows)
        weights, terms = pair_terms(logits, matched)
        if losses:
            loss_acc[...] = terms if first else loss_acc[...] + terms
        product = jnp.dot(weights.astype(jnp.bfloat16), right, preferred_element_type=jnp.float32)
        product = product.reshape(mine.size, rows, width)
        acc[...] = product if first else acc[...] + product

    def compute(s, mine, other, acc, losses):
        def act(gg):
            for m in range(other.size):
                for h in range(pieces):
                    other.arrived(gg, m, 1 - c, h)
            gradient(mine, other, acc, gg, s == 0, losses)

        each_chunk(s, act)

    def partial(acc, part, send, recv, side, k):
        other = lax.rem(side.me + k, side.size)
        return pltpu.make_async_remote_copy(
            src_ref=acc.at[other], dst_ref=part.at[side.me], send_sem=send.at[k - 1], recv_sem=recv.at[side.me],
            device_id={"dev": side.partner(other)}, device_id_type=MESH,
        )

    def partial_in(acc, part, send, recv, side, k):
        other = lax.rem(side.me + k, side.size)
        return pltpu.make_async_remote_copy(
            src_ref=acc.at[other], dst_ref=part.at[other], send_sem=send.at[k - 1], recv_sem=recv.at[other],
            device_id={"dev": side.partner(other)}, device_id_type=MESH,
        )

    def send_partials(acc, part, send, recv, side):
        for k in range(1, side.size):
            partial(acc, part, send, recv, side, k).start()

    def loss_copy(own, gathered, send, recv, axis, me, size, k, slot):
        return pltpu.make_async_remote_copy(
            src_ref=own, dst_ref=gathered.at[slot], send_sem=send.at[k - 1], recv_sem=recv.at[slot],
            device_id={axis: lax.rem(me + k, size)}, device_id_type=MESH,
        )

    def loss_out(value, own, gathered, send, recv, axis, me, size):
        own[...] = value
        gathered[me] = value
        for k in range(1, size):
            loss_copy(own, gathered, send, recv, axis, me, size, k, me).start()

    def loss_in(own, gathered, send, recv, axis, me, size):
        for k in range(1, size):
            loss_copy(own, gathered, send, recv, axis, me, size, k, lax.rem(me + k, size)).wait_recv()
        total = gathered[0]
        for k in range(1, size):
            total = total + gathered[k]
        return total

    over_dev = (loss_own, loss_dev, ld_send, ld_recv, "dev", d, members)
    over_grp = (loss_sum, loss_grp, lg_send, lg_recv, "grp", g, groups)
    text_part = (acc_t, part_t, pt_send, pt_recv, texts)
    image_part = (acc_i, part_i, pi_send, pi_recv, images)

    last = groups - 1
    for s in range(groups):
        if s:
            forward_z(s, texts)
            if s > 1:
                relay_plane(s - 1, images)
            compute(s - 1, texts, images, acc_t, False)
            forward_z(s, images)
        relay_plane(s, texts)
        if s == 0:
            relay_plane(s, images)
        compute(s, images, texts, acc_i, True)
    loss_out(jnp.full((8, 128), jnp.sum(loss_acc[...]), jnp.float32), *over_dev)
    send_partials(*image_part)
    if last:
        relay_plane(last, images)
    compute(last, texts, images, acc_t, False)
    send_partials(*text_part)
    loss_out(loss_in(*over_dev), *over_grp)
    loss_ref[...] = loss_in(*over_grp) * (1.0 / (rows * members * groups))

    for (acc, part, send, recv, side), out_ref in ((image_part, gi_ref), (text_part, gt_ref)):
        total = acc[side.me]
        for k in range(1, side.size):
            partial_in(acc, part, send, recv, side, k).wait_recv()
            total = total + part[lax.rem(side.me + k, side.size)]
        out_ref[...] = multiplier * total
        for k in range(1, side.size):
            partial(acc, part, send, recv, side, k).wait_send()
    for own, gathered, send, recv, axis, me, size in (over_dev, over_grp):
        for k in range(1, size):
            loss_copy(own, gathered, send, recv, axis, me, size, k, me).wait_send()

    for side in sides:
        for h in range(pieces):
            @pl.when(g + 1 < groups)
            def _():
                side.along_z(g, h, True, True).wait_send()

            @pl.when(g > 0)
            def _():
                side.along_z(g, h, False, True).wait_send()

            for s in range(groups):
                def act(gg):
                    for k in range(1, side.size):
                        side.to_plane(gg, k, h).wait_send()
                    for m in range(side.size):
                        side.to_core(gg, m, h).wait_send()

                each_chunk(s, act)
                for down in (False, True):
                    if s:
                        gg, there = from_side(s, down)

                        @pl.when(there & ((g > 0) if down else (g + 1 < groups)))
                        def _():
                            side.along_z(gg, h, not down).wait_send()


def write_out(gi_ref, gt_ref, loss_ref, gi_out, gt_out, loss_out):
    gi_out[...] = gi_ref[...]
    gt_out[...] = gt_ref[...]
    loss_out[0] = jnp.max(loss_ref[...])


def shards(groups, members, images, texts, logit_scale, logit_bias):
    rows, width = images.shape
    p_size, q_size = split_chips(members)
    pieces = piece_count(rows)
    f32, bf16 = jnp.float32, jnp.bfloat16
    dma = pltpu.SemaphoreType.DMA

    def side_sems(size):
        return [
            dma((groups, size, CORES, pieces)),
            dma((groups + 1, pieces)),
            dma((groups, max(size - 1, 1), pieces)),
            dma((groups, size, pieces)),
        ]

    held = (groups * (p_size + q_size) * CORES * 2 + (p_size + q_size) * 8) * rows * width
    vmem, smem = pl.BlockSpec(memory_space=pltpu.VMEM), pl.BlockSpec(memory_space=pltpu.SMEM)
    grad_image, grad_text, loss = pl.pallas_call(
        functools.partial(kernel, groups, p_size, q_size, pieces),
        out_shape=(
            jax.ShapeDtypeStruct((rows, width), f32),
            jax.ShapeDtypeStruct((rows, width), f32),
            jax.ShapeDtypeStruct((8, 128), f32),
        ),
        in_specs=[pl.BlockSpec(memory_space=pl.ANY)] * 4,
        out_specs=(vmem, vmem, vmem),
        scratch_shapes=[
            pltpu.VMEM((groups, p_size, CORES, rows, width), bf16),
            pltpu.VMEM((groups, q_size, CORES, rows, width), bf16),
            pltpu.VMEM((p_size, rows, width), f32),
            pltpu.VMEM((q_size, rows, width), f32),
            pltpu.VMEM((p_size, rows, width), f32),
            pltpu.VMEM((q_size, rows, width), f32),
            pltpu.VMEM((p_size * rows, q_size * CORES * rows), f32),
            pltpu.VMEM((8, 128), f32),
            pltpu.VMEM((members, 8, 128), f32),
            pltpu.VMEM((8, 128), f32),
            pltpu.VMEM((groups, 8, 128), f32),
            *side_sems(p_size),
            *side_sems(q_size),
            dma((p_size,)), dma((p_size,)), dma((q_size,)), dma((q_size,)),
            dma((members,)), dma((members,)), dma((groups,)), dma((groups,)),
            pltpu.SMEM((1,), f32), pltpu.SMEM((1,), f32), dma((4,)),
        ],
        compiler_params=pltpu.CompilerParams(
            collective_id=0, has_side_effects=True, vmem_limit_bytes=min(held + (members + groups) * 4096 + (12 << 20), 60 << 20)
        ),
    )(images, texts, logit_scale, logit_bias)
    return pl.pallas_call(
        write_out,
        out_shape=(
            jax.ShapeDtypeStruct((rows, width), f32),
            jax.ShapeDtypeStruct((rows, width), f32),
            jax.ShapeDtypeStruct((1,), f32),
        ),
        in_specs=[vmem, vmem, vmem],
        out_specs=(vmem, vmem, smem),
        compiler_params=pltpu.CompilerParams(vmem_limit_bytes=4 << 20),
    )(grad_image, grad_text, loss)


def solution(mesh):
    in_specs = (P(("grp", "dev"), None), P(("grp", "dev"), None), P(), P())
    out_specs = (P(("grp", "dev"), None), P(("grp", "dev"), None), P())
    body = functools.partial(shards, mesh.shape["grp"], mesh.shape["dev"])
    return jax.shard_map(body, mesh=mesh, in_specs=in_specs, out_specs=out_specs, check_vma=False)
```

```python
import functools
import math

import jax
import jax.numpy as jnp
from jax import lax
from jax.experimental import pallas as pl
from jax.experimental.pallas import tpu as pltpu
from jax.sharding import PartitionSpec as P

MESH = pl.DeviceIdType.MESH
CORES = 2


def split_chips(members):
    chips = members // CORES
    q_size = math.isqrt(chips)
    while chips % q_size:
        q_size -= 1
    return chips // q_size, q_size


def piece_count(rows):
    for pieces in (3, 2):
        if rows % (16 * pieces) == 0:
            return pieces
    return 1


def pair_terms(logits, matched):
    small = jnp.exp(-jnp.abs(logits))
    sigmoid = jnp.where(logits >= 0, 1.0, small) / (1.0 + small)
    if matched is None:
        return sigmoid, jnp.maximum(logits, 0.0) + jnp.log1p(small)
    weights = sigmoid - matched.astype(jnp.float32)
    signed = jnp.where(matched, -logits, logits)
    return weights, jnp.maximum(signed, 0.0) + jnp.log1p(small)


def kernel(
    groups, p_size, q_size, pieces,
    img_hbm, txt_hbm, scale_hbm, bias_hbm,
    gi_ref, gt_ref, loss_ref,
    img_all, txt_all, acc_i, acc_t, part_i, part_t,
    loss_acc, loss_own, loss_dev, loss_sum, loss_grp,
    img_recv, img_z, img_plane, img_core,
    txt_recv, txt_z, txt_plane, txt_core,
    pi_send, pi_recv, pt_send, pt_recv,
    ld_send, ld_recv, lg_send, lg_recv,
    scale_ref, bias_ref, fetch_sem,
):
    rows = img_hbm.shape[0]
    members = p_size * q_size * CORES
    g = lax.axis_index("grp")
    d = lax.axis_index("dev")
    c = lax.rem(d, CORES)
    chip = d // CORES
    q = lax.rem(chip, q_size)
    p = chip // q_size
    step_rows = rows // pieces

    def member(pi, qi, ci):
        return (pi * q_size + qi) * CORES + ci

    fetches = [
        pltpu.make_async_copy(src, dst, fetch_sem.at[i])
        for i, (src, dst) in enumerate((
            (txt_hbm, txt_all.at[g, q, c]), (img_hbm, img_all.at[g, p, c]), (scale_hbm, scale_ref), (bias_hbm, bias_ref),
        ))
    ]
    barrier = pltpu.get_barrier_semaphore()

    def greet(axis, index):
        pl.semaphore_signal(barrier, inc=1, device_id={axis: index}, device_id_type=MESH)

    @pl.when(g + 1 < groups)
    def _():
        greet("grp", g + 1)

    @pl.when(g > 0)
    def _():
        greet("grp", g - 1)

    for k in range(1, p_size):
        greet("dev", member(lax.rem(p + k, p_size), q, c))
    for k in range(1, q_size):
        greet("dev", member(p, lax.rem(q + k, q_size), c))
    greet("dev", member(p, q, 1 - c))
    for fetch in fetches:
        fetch.start()
    edges = (g > 0).astype(jnp.int32) + (g + 1 < groups).astype(jnp.int32)
    pl.semaphore_wait(barrier, p_size + q_size - 1 + edges)

    class Side:
        def __init__(self, all_ref, recv, zs, ps, cs, me, size, partner):
            self.all, self.recv = all_ref, recv
            self.zs, self.ps, self.cs = zs, ps, cs
            self.me, self.size, self.partner = me, size, partner

        def piece(self, gg, m, cc, h):
            return self.all.at[gg, m, cc, pl.ds(h * step_rows, step_rows)]

        def copy(self, gg, m, cc, h, send, target):
            dst = self.piece(gg, m, cc, h)
            return pltpu.make_async_remote_copy(
                src_ref=dst, dst_ref=dst, send_sem=send, recv_sem=self.recv.at[gg, m, cc, h],
                device_id=target, device_id_type=MESH,
            )

        def arrived(self, gg, m, cc, h):
            self.copy(gg, m, cc, h, self.cs.at[0, 0, 0], {"dev": member(p, q, 1 - c)}).wait_recv()

        def along_z(self, gg, h, up, own=False):
            slot = gg if (up or not own) else groups
            return self.copy(gg, self.me, c, h, self.zs.at[slot, h], {"grp": g + 1 if up else g - 1})

        def to_plane(self, gg, k, h):
            other = lax.rem(self.me + k, self.size)
            return self.copy(gg, self.me, c, h, self.ps.at[gg, k - 1, h], {"dev": self.partner(other)})

        def to_core(self, gg, m, h):
            return self.copy(gg, m, c, h, self.cs.at[gg, m, h], {"dev": member(p, q, 1 - c)})

    texts = Side(txt_all, txt_recv, txt_z, txt_plane, txt_core, q, q_size, lambda o: member(p, o, c))
    images = Side(img_all, img_recv, img_z, img_plane, img_core, p, p_size, lambda o: member(o, q, c))
    sides = (texts, images)

    def from_side(s, down):
        return (g - s, g >= s) if not down else (g + s, g + s < groups)

    for side, fetch in zip(sides, fetches):
        fetch.wait()
        for h in range(pieces):
            @pl.when(g + 1 < groups)
            def _():
                side.along_z(g, h, True, True).start()

            @pl.when(g > 0)
            def _():
                side.along_z(g, h, False, True).start()

            for k in range(1, side.size):
                side.to_plane(g, k, h).start()
            side.to_core(g, side.me, h).start()
    for fetch in fetches[2:]:
        fetch.wait()
    multiplier = scale_ref[0]
    offset = bias_ref[0]

    def forward_z(s, side):
        for h in range(pieces):
            for down in (False, True):
                gg, there = from_side(s, down)

                @pl.when(there)
                def _():
                    side.arrived(gg, side.me, c, h)

                    @pl.when((g > 0) if down else (g + 1 < groups))
                    def _():
                        side.along_z(gg, h, not down).start()

                    for k in range(1, side.size):
                        side.to_plane(gg, k, h).start()
                    side.to_core(gg, side.me, h).start()

    def each_chunk(s, act):
        if s == 0:
            act(g)
            return
        for down in (False, True):
            gg, there = from_side(s, down)

            @pl.when(there)
            def _():
                act(gg)

    def relay_plane(s, side):
        def act(gg):
            for h in range(pieces):
                for k in range(1, side.size):
                    other = lax.rem(side.me + k, side.size)
                    side.arrived(gg, other, c, h)
                    side.to_core(gg, other, h).start()

        each_chunk(s, act)

    def gradient(mine, other, acc, gg, first, losses):
        width = acc.shape[2]
        left = mine.all[g, :, c].reshape(mine.size * rows, width)
        right = other.all[gg].reshape(other.size * CORES * rows, width)
        logits = lax.dot_general(left, right, (((1,), (1,)), ((), ())), preferred_element_type=jnp.float32)
        logits = logits * multiplier + offset
        matched = None
        if first:
            row = lax.broadcasted_iota(jnp.int32, logits.shape, 0) - mine.me * rows
            col = lax.broadcasted_iota(jnp.int32, logits.shape, 1) - (other.me * CORES + c) * rows
            matched = (row == col) & (row >= 0) & (row < rows)
        weights, terms = pair_terms(logits, matched)
        if losses:
            loss_acc[...] = terms if first else loss_acc[...] + terms
        product = jnp.dot(weights.astype(jnp.bfloat16), right, preferred_element_type=jnp.float32)
        product = product.reshape(mine.size, rows, width)
        acc[...] = product if first else acc[...] + product

    def compute(s, mine, other, acc, losses):
        def act(gg):
            for m in range(other.size):
                for h in range(pieces):
                    other.arrived(gg, m, 1 - c, h)
            gradient(mine, other, acc, gg, s == 0, losses)

        each_chunk(s, act)

    def partial(acc, part, send, recv, side, k):
        other = lax.rem(side.me + k, side.size)
        return pltpu.make_async_remote_copy(
            src_ref=acc.at[other], dst_ref=part.at[side.me], send_sem=send.at[k - 1], recv_sem=recv.at[side.me],
            device_id={"dev": side.partner(other)}, device_id_type=MESH,
        )

    def partial_in(acc, part, send, recv, side, k):
        other = lax.rem(side.me + k, side.size)
        return pltpu.make_async_remote_copy(
            src_ref=acc.at[other], dst_ref=part.at[other], send_sem=send.at[k - 1], recv_sem=recv.at[other],
            device_id={"dev": side.partner(other)}, device_id_type=MESH,
        )

    def send_partials(acc, part, send, recv, side):
        for k in range(1, side.size):
            partial(acc, part, send, recv, side, k).start()

    def loss_copy(own, gathered, send, recv, axis, me, size, k, slot):
        return pltpu.make_async_remote_copy(
            src_ref=own, dst_ref=gathered.at[slot], send_sem=send.at[k - 1], recv_sem=recv.at[slot],
            device_id={axis: lax.rem(me + k, size)}, device_id_type=MESH,
        )

    def loss_out(value, own, gathered, send, recv, axis, me, size):
        own[...] = value
        gathered[me] = value
        for k in range(1, size):
            loss_copy(own, gathered, send, recv, axis, me, size, k, me).start()

    def loss_in(own, gathered, send, recv, axis, me, size):
        for k in range(1, size):
            loss_copy(own, gathered, send, recv, axis, me, size, k, lax.rem(me + k, size)).wait_recv()
        total = gathered[0]
        for k in range(1, size):
            total = total + gathered[k]
        return total

    over_dev = (loss_own, loss_dev, ld_send, ld_recv, "dev", d, members)
    over_grp = (loss_sum, loss_grp, lg_send, lg_recv, "grp", g, groups)
    text_part = (acc_t, part_t, pt_send, pt_recv, texts)
    image_part = (acc_i, part_i, pi_send, pi_recv, images)

    last = groups - 1
    for s in range(1, groups):
        forward_z(s, texts)
        forward_z(s, images)
        relay_plane(s - 1, texts)
        relay_plane(s - 1, images)
        compute(s - 1, images, texts, acc_i, True)
        compute(s - 1, texts, images, acc_t, False)
    relay_plane(last, texts)
    relay_plane(last, images)
    compute(last, images, texts, acc_i, True)
    loss_out(jnp.full((8, 128), jnp.sum(loss_acc[...]), jnp.float32), *over_dev)
    send_partials(*image_part)
    compute(last, texts, images, acc_t, False)
    send_partials(*text_part)
    loss_out(loss_in(*over_dev), *over_grp)
    loss_ref[...] = loss_in(*over_grp) * (1.0 / (rows * members * groups))

    for (acc, part, send, recv, side), out_ref in ((image_part, gi_ref), (text_part, gt_ref)):
        total = acc[side.me]
        for k in range(1, side.size):
            partial_in(acc, part, send, recv, side, k).wait_recv()
            total = total + part[lax.rem(side.me + k, side.size)]
        out_ref[...] = multiplier * total
        for k in range(1, side.size):
            partial(acc, part, send, recv, side, k).wait_send()
    for own, gathered, send, recv, axis, me, size in (over_dev, over_grp):
        for k in range(1, size):
            loss_copy(own, gathered, send, recv, axis, me, size, k, me).wait_send()

    for side in sides:
        for h in range(pieces):
            @pl.when(g + 1 < groups)
            def _():
                side.along_z(g, h, True, True).wait_send()

            @pl.when(g > 0)
            def _():
                side.along_z(g, h, False, True).wait_send()

            for s in range(groups):
                def act(gg):
                    for k in range(1, side.size):
                        side.to_plane(gg, k, h).wait_send()
                    for m in range(side.size):
                        side.to_core(gg, m, h).wait_send()

                each_chunk(s, act)
                for down in (False, True):
                    if s:
                        gg, there = from_side(s, down)

                        @pl.when(there & ((g > 0) if down else (g + 1 < groups)))
                        def _():
                            side.along_z(gg, h, not down).wait_send()


def write_out(gi_ref, gt_ref, loss_ref, gi_out, gt_out, loss_out):
    gi_out[...] = gi_ref[...]
    gt_out[...] = gt_ref[...]
    loss_out[0] = jnp.max(loss_ref[...])


def shards(groups, members, images, texts, logit_scale, logit_bias):
    rows, width = images.shape
    p_size, q_size = split_chips(members)
    pieces = piece_count(rows)
    f32, bf16 = jnp.float32, jnp.bfloat16
    dma = pltpu.SemaphoreType.DMA

    def side_sems(size):
        return [
            dma((groups, size, CORES, pieces)),
            dma((groups + 1, pieces)),
            dma((groups, max(size - 1, 1), pieces)),
            dma((groups, size, pieces)),
        ]

    held = (groups * (p_size + q_size) * CORES * 2 + (p_size + q_size) * 8) * rows * width
    vmem, smem = pl.BlockSpec(memory_space=pltpu.VMEM), pl.BlockSpec(memory_space=pltpu.SMEM)
    grad_image, grad_text, loss = pl.pallas_call(
        functools.partial(kernel, groups, p_size, q_size, pieces),
        out_shape=(
            jax.ShapeDtypeStruct((rows, width), f32),
            jax.ShapeDtypeStruct((rows, width), f32),
            jax.ShapeDtypeStruct((8, 128), f32),
        ),
        in_specs=[pl.BlockSpec(memory_space=pl.ANY)] * 4,
        out_specs=(vmem, vmem, vmem),
        scratch_shapes=[
            pltpu.VMEM((groups, p_size, CORES, rows, width), bf16),
            pltpu.VMEM((groups, q_size, CORES, rows, width), bf16),
            pltpu.VMEM((p_size, rows, width), f32),
            pltpu.VMEM((q_size, rows, width), f32),
            pltpu.VMEM((p_size, rows, width), f32),
            pltpu.VMEM((q_size, rows, width), f32),
            pltpu.VMEM((p_size * rows, q_size * CORES * rows), f32),
            pltpu.VMEM((8, 128), f32),
            pltpu.VMEM((members, 8, 128), f32),
            pltpu.VMEM((8, 128), f32),
            pltpu.VMEM((groups, 8, 128), f32),
            *side_sems(p_size),
            *side_sems(q_size),
            dma((p_size,)), dma((p_size,)), dma((q_size,)), dma((q_size,)),
            dma((members,)), dma((members,)), dma((groups,)), dma((groups,)),
            pltpu.SMEM((1,), f32), pltpu.SMEM((1,), f32), dma((4,)),
        ],
        compiler_params=pltpu.CompilerParams(
            collective_id=0, has_side_effects=True, vmem_limit_bytes=min(held + (members + groups) * 4096 + (12 << 20), 60 << 20)
        ),
    )(images, texts, logit_scale, logit_bias)
    return pl.pallas_call(
        write_out,
        out_shape=(
            jax.ShapeDtypeStruct((rows, width), f32),
            jax.ShapeDtypeStruct((rows, width), f32),
            jax.ShapeDtypeStruct((1,), f32),
        ),
        in_specs=[vmem, vmem, vmem],
        out_specs=(vmem, vmem, smem),
        compiler_params=pltpu.CompilerParams(vmem_limit_bytes=4 << 20),
    )(grad_image, grad_text, loss)


def solution(mesh):
    in_specs = (P(("grp", "dev"), None), P(("grp", "dev"), None), P(), P())
    out_specs = (P(("grp", "dev"), None), P(("grp", "dev"), None), P())
    body = functools.partial(shards, mesh.shape["grp"], mesh.shape["dev"])
    return jax.shard_map(body, mesh=mesh, in_specs=in_specs, out_specs=out_specs, check_vma=False)
```

```python
import functools
import math

import jax
import jax.numpy as jnp
from jax import lax
from jax.experimental import pallas as pl
from jax.experimental.pallas import tpu as pltpu
from jax.sharding import PartitionSpec as P

MESH = pl.DeviceIdType.MESH
CORES = 2


def split_chips(members):
    chips = members // CORES
    q_size = math.isqrt(chips)
    while chips % q_size:
        q_size -= 1
    return chips // q_size, q_size


def piece_count(rows):
    for pieces in (3, 2):
        if rows % (16 * pieces) == 0:
            return pieces
    return 1


def pair_terms(logits, matched):
    small = jnp.exp(-jnp.abs(logits))
    sigmoid = jnp.where(logits >= 0, 1.0, small) / (1.0 + small)
    if matched is None:
        return sigmoid, jnp.maximum(logits, 0.0) + jnp.log1p(small)
    weights = sigmoid - matched.astype(jnp.float32)
    signed = jnp.where(matched, -logits, logits)
    return weights, jnp.maximum(signed, 0.0) + jnp.log1p(small)


def kernel(
    groups, p_size, q_size, pieces,
    img_hbm, txt_hbm, scale_hbm, bias_hbm,
    gi_ref, gt_ref, loss_ref,
    img_all, txt_all, acc_i, acc_t, part_i, part_t,
    loss_acc, loss_own, loss_dev, loss_sum, loss_grp,
    img_recv, img_z, img_plane, img_core,
    txt_recv, txt_z, txt_plane, txt_core,
    pi_send, pi_recv, pt_send, pt_recv,
    ld_send, ld_recv, lg_send, lg_recv,
    scale_ref, bias_ref, fetch_sem,
):
    rows = img_hbm.shape[0]
    members = p_size * q_size * CORES
    g = lax.axis_index("grp")
    d = lax.axis_index("dev")
    c = lax.rem(d, CORES)
    chip = d // CORES
    q = lax.rem(chip, q_size)
    p = chip // q_size
    step_rows = rows // pieces

    def member(pi, qi, ci):
        return (pi * q_size + qi) * CORES + ci

    fetches = [
        pltpu.make_async_copy(src, dst, fetch_sem.at[i])
        for i, (src, dst) in enumerate((
            (txt_hbm, txt_all.at[g, q, c]), (img_hbm, img_all.at[g, p, c]), (scale_hbm, scale_ref), (bias_hbm, bias_ref),
        ))
    ]
    barrier = pltpu.get_barrier_semaphore()

    def greet(axis, index):
        pl.semaphore_signal(barrier, inc=1, device_id={axis: index}, device_id_type=MESH)

    @pl.when(g + 1 < groups)
    def _():
        greet("grp", g + 1)

    @pl.when(g > 0)
    def _():
        greet("grp", g - 1)

    for k in range(1, p_size):
        greet("dev", member(lax.rem(p + k, p_size), q, c))
    for k in range(1, q_size):
        greet("dev", member(p, lax.rem(q + k, q_size), c))
    greet("dev", member(p, q, 1 - c))
    for fetch in fetches:
        fetch.start()
    edges = (g > 0).astype(jnp.int32) + (g + 1 < groups).astype(jnp.int32)
    pl.semaphore_wait(barrier, p_size + q_size - 1 + edges)

    class Side:
        def __init__(self, all_ref, recv, zs, ps, cs, me, size, partner):
            self.all, self.recv = all_ref, recv
            self.zs, self.ps, self.cs = zs, ps, cs
            self.me, self.size, self.partner = me, size, partner

        def piece(self, gg, m, cc, h):
            return self.all.at[gg, m, cc, pl.ds(h * step_rows, step_rows)]

        def copy(self, gg, m, cc, h, send, target):
            dst = self.piece(gg, m, cc, h)
            return pltpu.make_async_remote_copy(
                src_ref=dst, dst_ref=dst, send_sem=send, recv_sem=self.recv.at[gg, m, cc, h],
                device_id=target, device_id_type=MESH,
            )

        def arrived(self, gg, m, cc, h):
            self.copy(gg, m, cc, h, self.cs.at[0, 0, 0], {"dev": member(p, q, 1 - c)}).wait_recv()

        def along_z(self, gg, h, up, own=False):
            slot = gg if (up or not own) else groups
            return self.copy(gg, self.me, c, h, self.zs.at[slot, h], {"grp": g + 1 if up else g - 1})

        def to_plane(self, gg, k, h):
            other = lax.rem(self.me + k, self.size)
            return self.copy(gg, self.me, c, h, self.ps.at[gg, k - 1, h], {"dev": self.partner(other)})

        def to_core(self, gg, m, h):
            return self.copy(gg, m, c, h, self.cs.at[gg, m, h], {"dev": member(p, q, 1 - c)})

    texts = Side(txt_all, txt_recv, txt_z, txt_plane, txt_core, q, q_size, lambda o: member(p, o, c))
    images = Side(img_all, img_recv, img_z, img_plane, img_core, p, p_size, lambda o: member(o, q, c))
    sides = (texts, images)

    def from_side(s, down):
        return (g - s, g >= s) if not down else (g + s, g + s < groups)

    for side, fetch in zip(sides, fetches):
        fetch.wait()
        for h in range(pieces):
            @pl.when(g + 1 < groups)
            def _():
                side.along_z(g, h, True, True).start()

            @pl.when(g > 0)
            def _():
                side.along_z(g, h, False, True).start()

            for k in range(1, side.size):
                side.to_plane(g, k, h).start()
            side.to_core(g, side.me, h).start()
    for fetch in fetches[2:]:
        fetch.wait()
    multiplier = scale_ref[0]
    offset = bias_ref[0]

    def forward_z(s, side):
        for h in range(pieces):
            for down in (False, True):
                gg, there = from_side(s, down)

                @pl.when(there)
                def _():
                    side.arrived(gg, side.me, c, h)

                    @pl.when((g > 0) if down else (g + 1 < groups))
                    def _():
                        side.along_z(gg, h, not down).start()

                    for k in range(1, side.size):
                        side.to_plane(gg, k, h).start()
                    side.to_core(gg, side.me, h).start()

    def each_chunk(s, act):
        if s == 0:
            act(g)
            return
        for down in (False, True):
            gg, there = from_side(s, down)

            @pl.when(there)
            def _():
                act(gg)

    def relay_plane(s, side):
        def act(gg):
            for h in range(pieces):
                for k in range(1, side.size):
                    other = lax.rem(side.me + k, side.size)
                    side.arrived(gg, other, c, h)
                    side.to_core(gg, other, h).start()

        each_chunk(s, act)

    def gradient(mine, other, acc, gg, first, losses):
        width = acc.shape[2]
        left = mine.all[g, :, c].reshape(mine.size * rows, width)
        right = other.all[gg].reshape(other.size * CORES * rows, width)
        logits = lax.dot_general(left, right, (((1,), (1,)), ((), ())), preferred_element_type=jnp.float32)
        logits = logits * multiplier + offset
        matched = None
        if first:
            row = lax.broadcasted_iota(jnp.int32, logits.shape, 0) - mine.me * rows
            col = lax.broadcasted_iota(jnp.int32, logits.shape, 1) - (other.me * CORES + c) * rows
            matched = (row == col) & (row >= 0) & (row < rows)
        weights, terms = pair_terms(logits, matched)
        if losses:
            loss_acc[...] = terms if first else loss_acc[...] + terms
        product = jnp.dot(weights.astype(jnp.bfloat16), right, preferred_element_type=jnp.float32)
        product = product.reshape(mine.size, rows, width)
        acc[...] = product if first else acc[...] + product

    def compute(s, mine, other, acc, losses):
        def act(gg):
            for m in range(other.size):
                for h in range(pieces):
                    other.arrived(gg, m, 1 - c, h)
            gradient(mine, other, acc, gg, s == 0, losses)

        each_chunk(s, act)

    def partial(acc, part, send, recv, side, k):
        other = lax.rem(side.me + k, side.size)
        return pltpu.make_async_remote_copy(
            src_ref=acc.at[other], dst_ref=part.at[side.me], send_sem=send.at[k - 1], recv_sem=recv.at[side.me],
            device_id={"dev": side.partner(other)}, device_id_type=MESH,
        )

    def partial_in(acc, part, send, recv, side, k):
        other = lax.rem(side.me + k, side.size)
        return pltpu.make_async_remote_copy(
            src_ref=acc.at[other], dst_ref=part.at[other], send_sem=send.at[k - 1], recv_sem=recv.at[other],
            device_id={"dev": side.partner(other)}, device_id_type=MESH,
        )

    def send_partials(acc, part, send, recv, side):
        for k in range(1, side.size):
            partial(acc, part, send, recv, side, k).start()

    def loss_copy(own, gathered, send, recv, axis, me, size, k, slot):
        return pltpu.make_async_remote_copy(
            src_ref=own, dst_ref=gathered.at[slot], send_sem=send.at[k - 1], recv_sem=recv.at[slot],
            device_id={axis: lax.rem(me + k, size)}, device_id_type=MESH,
        )

    def loss_out(value, own, gathered, send, recv, axis, me, size):
        own[...] = value
        gathered[me] = value
        for k in range(1, size):
            loss_copy(own, gathered, send, recv, axis, me, size, k, me).start()

    def loss_in(own, gathered, send, recv, axis, me, size):
        for k in range(1, size):
            loss_copy(own, gathered, send, recv, axis, me, size, k, lax.rem(me + k, size)).wait_recv()
        total = gathered[0]
        for k in range(1, size):
            total = total + gathered[k]
        return total

    over_dev = (loss_own, loss_dev, ld_send, ld_recv, "dev", d, members)
    over_grp = (loss_sum, loss_grp, lg_send, lg_recv, "grp", g, groups)
    text_part = (acc_t, part_t, pt_send, pt_recv, texts)
    image_part = (acc_i, part_i, pi_send, pi_recv, images)

    last = groups - 1
    for s in range(1, groups):
        forward_z(s, texts)
        forward_z(s, images)
        relay_plane(s - 1, texts)
        relay_plane(s - 1, images)
        compute(s - 1, images, texts, acc_i, True)
        compute(s - 1, texts, images, acc_t, False)
    relay_plane(last, texts)
    relay_plane(last, images)
    compute(last, images, texts, acc_i, True)
    loss_out(jnp.full((8, 128), jnp.sum(loss_acc[...]), jnp.float32), *over_dev)
    send_partials(*image_part)
    compute(last, texts, images, acc_t, False)
    send_partials(*text_part)
    loss_out(loss_in(*over_dev), *over_grp)
    loss_ref[...] = loss_in(*over_grp) * (1.0 / (rows * members * groups))

    for (acc, part, send, recv, side), out_ref in ((image_part, gi_ref), (text_part, gt_ref)):
        total = acc[side.me]
        for k in range(1, side.size):
            partial_in(acc, part, send, recv, side, k).wait_recv()
            total = total + part[lax.rem(side.me + k, side.size)]
        out_ref[...] = multiplier * total
        for k in range(1, side.size):
            partial(acc, part, send, recv, side, k).wait_send()
    for own, gathered, send, recv, axis, me, size in (over_dev, over_grp):
        for k in range(1, size):
            loss_copy(own, gathered, send, recv, axis, me, size, k, me).wait_send()

    for side in sides:
        for h in range(pieces):
            @pl.when(g + 1 < groups)
            def _():
                side.along_z(g, h, True, True).wait_send()

            @pl.when(g > 0)
            def _():
                side.along_z(g, h, False, True).wait_send()

            for s in range(groups):
                def act(gg):
                    for k in range(1, side.size):
                        side.to_plane(gg, k, h).wait_send()
                    for m in range(side.size):
                        side.to_core(gg, m, h).wait_send()

                each_chunk(s, act)
                for down in (False, True):
                    if s:
                        gg, there = from_side(s, down)

                        @pl.when(there & ((g > 0) if down else (g + 1 < groups)))
                        def _():
                            side.along_z(gg, h, not down).wait_send()


def write_out(gi_ref, gt_ref, loss_ref, gi_out, gt_out, loss_out):
    gi_out[...] = gi_ref[...]
    gt_out[...] = gt_ref[...]
    loss_out[0] = jnp.max(loss_ref[...])


def shards(groups, members, images, texts, logit_scale, logit_bias):
    rows, width = images.shape
    p_size, q_size = split_chips(members)
    pieces = piece_count(rows)
    f32, bf16 = jnp.float32, jnp.bfloat16
    dma = pltpu.SemaphoreType.DMA

    def side_sems(size):
        return [
            dma((groups, size, CORES, pieces)),
            dma((groups + 1, pieces)),
            dma((groups, max(size - 1, 1), pieces)),
            dma((groups, size, pieces)),
        ]

    held = (groups * (p_size + q_size) * CORES * 2 + (p_size + q_size) * 8) * rows * width
    vmem, smem = pl.BlockSpec(memory_space=pltpu.VMEM), pl.BlockSpec(memory_space=pltpu.SMEM)
    grad_image, grad_text, loss = pl.pallas_call(
        functools.partial(kernel, groups, p_size, q_size, pieces),
        out_shape=(
            jax.ShapeDtypeStruct((rows, width), f32),
            jax.ShapeDtypeStruct((rows, width), f32),
            jax.ShapeDtypeStruct((8, 128), f32),
        ),
        in_specs=[pl.BlockSpec(memory_space=pl.ANY)] * 4,
        out_specs=(vmem, vmem, vmem),
        scratch_shapes=[
            pltpu.VMEM((groups, p_size, CORES, rows, width), bf16),
            pltpu.VMEM((groups, q_size, CORES, rows, width), bf16),
            pltpu.VMEM((p_size, rows, width), f32),
            pltpu.VMEM((q_size, rows, width), f32),
            pltpu.VMEM((p_size, rows, width), f32),
            pltpu.VMEM((q_size, rows, width), f32),
            pltpu.VMEM((p_size * rows, q_size * CORES * rows), f32),
            pltpu.VMEM((8, 128), f32),
            pltpu.VMEM((members, 8, 128), f32),
            pltpu.VMEM((8, 128), f32),
            pltpu.VMEM((groups, 8, 128), f32),
            *side_sems(p_size),
            *side_sems(q_size),
            dma((p_size,)), dma((p_size,)), dma((q_size,)), dma((q_size,)),
            dma((members,)), dma((members,)), dma((groups,)), dma((groups,)),
            pltpu.SMEM((1,), f32), pltpu.SMEM((1,), f32), dma((4,)),
        ],
        compiler_params=pltpu.CompilerParams(
            collective_id=0, has_side_effects=True, vmem_limit_bytes=min(held + (members + groups) * 4096 + (12 << 20), 60 << 20)
        ),
    )(pltpu.with_memory_space_constraint(images, pltpu.HBM), pltpu.with_memory_space_constraint(texts, pltpu.HBM), logit_scale, logit_bias)
    return pl.pallas_call(
        write_out,
        out_shape=(
            jax.ShapeDtypeStruct((rows, width), f32),
            jax.ShapeDtypeStruct((rows, width), f32),
            jax.ShapeDtypeStruct((1,), f32),
        ),
        in_specs=[vmem, vmem, vmem],
        out_specs=(vmem, vmem, smem),
        compiler_params=pltpu.CompilerParams(vmem_limit_bytes=4 << 20),
    )(grad_image, grad_text, loss)


def solution(mesh):
    in_specs = (P(("grp", "dev"), None), P(("grp", "dev"), None), P(), P())
    out_specs = (P(("grp", "dev"), None), P(("grp", "dev"), None), P())
    body = functools.partial(shards, mesh.shape["grp"], mesh.shape["dev"])
    return jax.shard_map(body, mesh=mesh, in_specs=in_specs, out_specs=out_specs, check_vma=False)
```
